32 devices in a mesh: channel: 4 (over z), tm: 4 (over y, core), beam: 2 (over x).
Axes of the slice: x: 2, y: 2, z: 4, core: 2. Of those that a mesh axis runs over, the one named last changes fastest.
Arguments:
- voltages: bfloat16 [2, 2048, 64, 1024], P(None, ('beam', 'channel'), None, 'tm'), may hold values from -6 to 6
- positions: int32 [2048], replicated, may hold values from 0 to 1023
- delays: int32 [32, 1024], P(None, 'channel'), may hold values from 0 to 63
Outputs:
- intensity: float32 [1024, 64, 1024], P(('beam', 'tm'), 'channel')
- dedispersed: float32 [1024, 32, 64], P(('beam', 'tm'), 'channel')
The draws below stay inside these ranges and needn't reach their ends.
Inputs may be any that keep to these rules, and one draw needn't show every extreme that they name: `positions`: place on a grid of 4 cylinders by 256 places along each.
All inputs are finite; a program needn't handle non-finite values.
Results may differ from the reference program's by a relative error of at most 0.0071.
Values may be sent and summed in bfloat16 or wider, within the bound.
No kernel may reach another device: no remote copies, remote signals or barrier semaphores. Data moves between devices by JAX's collectives and lax.ppermute only.
A program may use at most 192 MiB of HBM per device.

```python
import math
import jax
import jax.numpy as jnp
from jax import lax

FEEDS = 2048
CHANNELS = 64
BEAMS = 1024
UPCH = 16
TAPS = 8
SAMPLES = 1024
FRAMES = 64
FINE = 1024
DM = 32


def touch_ends(array, rng, low, high):
    shape = array.shape
    place = [jax.random.randint(jax.random.fold_in(rng, axis), (), 0, shape[axis]) for axis in range(len(shape))]
    array = array.at[tuple(place)].set(low)
    longest = shape.index(max(shape))
    place[longest] = (place[longest] + 1) % shape[longest]
    return array.at[tuple(place)].set(high)


def levels(stream_key, extent, pieces, smallest, largest):
    def one(position, parts):
        steps = jax.random.uniform(jax.random.fold_in(jax.random.fold_in(stream_key, 6), position), (parts,), jnp.float32, smallest / len(pieces), largest / len(pieces))
        return jnp.repeat(jnp.exp(steps), extent[position] // parts).reshape((-1,) + (1,) * (len(extent) - position - 1))

    gain = one(*pieces[0])
    for cut in pieces[1:]:
        gain = gain * one(*cut)
    return gain


def gaussian(stream_key, dims, deviation, bound, pieces=(), held_as=jnp.bfloat16):
    entries = deviation * jax.random.normal(stream_key, dims, jnp.float32)
    if pieces:
        entries = entries * levels(stream_key, dims, pieces, -0.22, 0.18)
    return jnp.clip(entries, -bound, bound).astype(held_as)


def setup_inputs(seed: int = 0) -> dict:
    streams_of = jax.random.split(jax.random.key(seed), 4)
    voltages = gaussian(streams_of[0], (2, FEEDS, CHANNELS, SAMPLES), 1.0, 6.0, ((1, 8), (3, 4)))
    positions = touch_ends(jax.random.randint(streams_of[1], (FEEDS,), 0, BEAMS), jax.random.fold_in(streams_of[1], 1), 0, BEAMS - 1).astype(jnp.int32)
    delays = touch_ends(jax.random.randint(streams_of[2], (DM, FINE), 0, FRAMES), jax.random.fold_in(streams_of[2], 1), 0, FRAMES - 1).astype(jnp.int32)
    return {"voltages": voltages, "positions": positions, "delays": delays}


TWO_PI = 2.0 * math.pi
HIGHEST = lax.Precision.HIGHEST

def window_table(tap_count, upch_factor):
    length = tap_count * upch_factor
    sample_index = jnp.arange(length).astype(jnp.float32)
    taper = jnp.sinc((sample_index - (length - 1) / 2.0) / upch_factor) * (0.5 - 0.5 * jnp.cos(TWO_PI * (sample_index + 0.5) / length))
    taper = taper / jnp.sqrt(jnp.sum(taper * taper))
    return taper.reshape(tap_count, upch_factor)

def steering(positions, beam_start, item_count, places, feed_count):
    beam_ids = beam_start + jnp.arange(item_count).astype(jnp.int32)
    beam_east = beam_ids // places
    beam_north = beam_ids % places
    cylinder = positions // places
    along_row = positions % places
    coarse = beam_east[:, None] * cylinder[None, :] % 4
    north_turns = beam_north[:, None] * along_row[None, :] % places
    angles = TWO_PI * (coarse.astype(jnp.float32) / 4.0 + north_turns.astype(jnp.float32) / places)
    norm_scale = 1.0 / math.sqrt(feed_count)
    w_real = (jnp.cos(angles) * norm_scale).astype(jnp.bfloat16)
    w_imag = (-jnp.sin(angles) * norm_scale).astype(jnp.bfloat16)
    top_half = jnp.concatenate([w_real, -w_imag], axis=1)
    low_half = jnp.concatenate([w_imag, w_real], axis=1)
    return jnp.concatenate([top_half, low_half], axis=0)

def reference(voltages, positions, delays):
    feed_count = voltages.shape[1]
    sample_count = voltages.shape[3]
    frame_count = sample_count // UPCH
    places = BEAMS // 4
    rim_width = (TAPS - 1) * UPCH
    weights = steering(positions, 0, BEAMS, places, feed_count)
    window = window_table(TAPS, UPCH)
    indices = jnp.arange(UPCH).astype(jnp.int32)
    phases = (indices[:, None] * indices[None, :] % UPCH).astype(jnp.float32) * (TWO_PI / UPCH)
    dft_real = jnp.cos(phases)
    dft_imag = -jnp.sin(phases)

    def channel_power(channel_data):
        stacked = channel_data.reshape(2 * feed_count, sample_count)
        formed = jnp.dot(weights, stacked, preferred_element_type=jnp.float32).astype(jnp.bfloat16)
        formed = formed.reshape(2, BEAMS, sample_count)
        padded = jnp.concatenate([jnp.zeros((2, BEAMS, rim_width), jnp.bfloat16), formed], axis=2)
        filtered = jnp.zeros((2, BEAMS, sample_count), jnp.float32)
        for tap_index in range(TAPS):
            filtered = filtered + padded[:, :, tap_index * UPCH:tap_index * UPCH + sample_count] * jnp.tile(window[tap_index], frame_count)
        halves = filtered.reshape(2, BEAMS, frame_count, UPCH)
        spec_real = jnp.einsum('bnm,mk->bnk', halves[0], dft_real, precision=HIGHEST) - jnp.einsum('bnm,mk->bnk', halves[1], dft_imag, precision=HIGHEST)
        spec_imag = jnp.einsum('bnm,mk->bnk', halves[0], dft_imag, precision=HIGHEST) + jnp.einsum('bnm,mk->bnk', halves[1], dft_real, precision=HIGHEST)
        return (spec_real * spec_real + spec_imag * spec_imag).reshape(BEAMS, sample_count)
    power_grid = lax.map(channel_power, jnp.moveaxis(voltages, 2, 0))
    intensity = jnp.transpose(power_grid, (1, 0, 2))
    frame_grid = intensity.reshape(BEAMS, CHANNELS, frame_count, UPCH)
    centred = frame_grid - lax.optimization_barrier(jnp.mean(frame_grid, axis=2, keepdims=True))
    spectrum = jnp.fft.rfft(centred, axis=2)
    freq_bins = frame_count // 2 + 1
    left_real = jnp.transpose(jnp.real(spectrum), (2, 0, 1, 3)).reshape(freq_bins, BEAMS, FINE)
    left_imag = jnp.transpose(jnp.imag(spectrum), (2, 0, 1, 3)).reshape(freq_bins, BEAMS, FINE)
    delay_cols = jnp.transpose(delays)

    def trial_bin(bin_data):
        frequency, part_real, part_imag = bin_data
        angle_grid = (frequency * delay_cols % frame_count).astype(jnp.float32) * (TWO_PI / frame_count)
        cos_table = jnp.cos(angle_grid)
        sin_table = jnp.sin(angle_grid)
        out_real = jnp.dot(part_real, cos_table, precision=HIGHEST) + jnp.dot(part_imag, sin_table, precision=HIGHEST)
        out_imag = jnp.dot(part_imag, cos_table, precision=HIGHEST) - jnp.dot(part_real, sin_table, precision=HIGHEST)
        return (out_real, out_imag)
    trial_real, trial_imag = lax.map(trial_bin, (jnp.arange(freq_bins).astype(jnp.int32), left_real, left_imag))
    series = jnp.fft.irfft(trial_real + 1j * trial_imag, n=frame_count, axis=0)
    dedispersed = jnp.transpose(series, (1, 2, 0)) / math.sqrt(FINE)
    return (intensity, dedispersed)
```

```python
import functools
import math

import jax
import jax.numpy as jnp
import numpy as np
from jax import lax
from jax.experimental import pallas as pl
from jax.experimental.pallas import tpu as pltpu
from jax.sharding import PartitionSpec as P

BEAMS = 1024
UPCH = 16
TAPS = 8
FINE = 1024
LANES = 128

TWO_PI = 2.0 * math.pi


def ring(value, axis, shift):
    count = lax.axis_size(axis)
    return lax.ppermute(value, axis, [(i, (i + shift) % count) for i in range(count)])


def steering(positions, beam_ids, places, feed_count):
    beam_east = beam_ids // places
    beam_north = beam_ids % places
    cylinder = positions // places
    along_row = positions % places
    coarse = beam_east[:, None] * cylinder[None, :] % 4
    north_turns = beam_north[:, None] * along_row[None, :] % places
    angles = TWO_PI * (coarse.astype(jnp.float32) / 4.0 + north_turns.astype(jnp.float32) / places)
    norm_scale = 1.0 / math.sqrt(feed_count)
    w_real = (jnp.cos(angles) * norm_scale).astype(jnp.bfloat16)
    w_imag = (-jnp.sin(angles) * norm_scale).astype(jnp.bfloat16)
    return w_real, w_imag


def filter_matrices():
    length = TAPS * UPCH
    index = np.arange(length, dtype=np.float64)
    taper = np.sinc((index - (length - 1) / 2.0) / UPCH) * (
        0.5 - 0.5 * np.cos(TWO_PI * (index + 0.5) / length)
    )
    taper = taper / np.sqrt(np.sum(taper * taper))
    frames = LANES // UPCH
    mats = []
    for first in (-LANES, 0):
        sample = np.arange(first, first + LANES)
        inner = sample % UPCH
        tap = (sample - inner)[:, None] // UPCH - np.arange(frames)[None, :] + TAPS - 1
        inside = (tap >= 0) & (tap < TAPS)
        gain = np.where(inside, taper[np.clip(tap, 0, TAPS - 1) * UPCH + inner[:, None]], 0.0)
        phase = TWO_PI * (inner[:, None] * np.arange(UPCH)[None, :] % UPCH) / UPCH
        real = (gain[:, :, None] * np.cos(phase)[:, None, :]).reshape(LANES, LANES)
        imag = (gain[:, :, None] * -np.sin(phase)[:, None, :]).reshape(LANES, LANES)
        full = np.concatenate(
            [np.concatenate([real, imag], axis=1), np.concatenate([-imag, real], axis=1)], axis=0
        )
        high = full.astype(jnp.bfloat16)
        low = (full - high.astype(np.float64)).astype(jnp.bfloat16)
        mats.append(np.concatenate([high, low], axis=1))
    return np.stack(mats)


def frame_distance(frames):
    row = np.arange(frames)[:, None]
    col = np.arange(frames * UPCH)[None, :] // UPCH
    return ((row - col) % frames).astype(np.int32)


def partial_kernel(*refs):
    w_ref, *v_refs, out_ref = refs
    total = None
    for s, v_ref in enumerate(v_refs):
        part = jnp.dot(w_ref[s], v_ref[...], preferred_element_type=jnp.float32)
        total = part if total is None else total + part
    out_ref[...] = total.astype(out_ref.dtype)


def beam_partial(weights, pieces):
    sources, rows, cols = weights.shape
    chans, _, samples = pieces[0].shape
    return pl.pallas_call(
        partial_kernel,
        grid=(chans,),
        in_specs=[pl.BlockSpec((sources, rows, cols), lambda c: (0, 0, 0))]
        + [pl.BlockSpec((None, cols, samples), lambda c: (c, 0, 0)) for _ in pieces],
        out_specs=pl.BlockSpec((None, rows, samples), lambda c: (c, 0, 0)),
        out_shape=jax.ShapeDtypeStruct((chans, rows, samples), jnp.bfloat16),
        name="beam_partial",
        cost_estimate=pl.CostEstimate(
            flops=2 * chans * rows * sources * cols * samples,
            bytes_accessed=2 * (sources * rows * cols + chans * samples * (sources * cols + rows)),
            transcendentals=0,
        ),
    )(weights, *pieces)


def own_kernel(n_pieces, n_received, *refs):
    w_ref = refs[0]
    v_refs = refs[1 : 1 + n_pieces]
    r_refs = refs[1 + n_pieces : 1 + n_pieces + n_received]
    out_refs = refs[1 + n_pieces + n_received :]
    total = None
    for s, v_ref in enumerate(v_refs):
        part = jnp.dot(w_ref[s], v_ref[...], preferred_element_type=jnp.float32)
        total = part if total is None else total + part
    for r_ref in r_refs:
        total = total + r_ref[...].astype(jnp.float32)
    beams = total.astype(jnp.bfloat16)
    held = beams.shape[0] // 2
    each = held // len(out_refs)
    for j, out_ref in enumerate(out_refs):
        for a in range(out_ref.shape[0]):
            lanes = slice(a * LANES, (a + 1) * LANES)
            out_ref[a, :, :LANES] = beams[j * each : (j + 1) * each, lanes]
            out_ref[a, :, LANES:] = beams[held + j * each : held + (j + 1) * each, lanes]


def own_beams(weights, pieces, received, blocks):
    sources, rows, cols = weights.shape
    chans, _, samples = pieces[0].shape
    each = rows // 2 // blocks
    tiles = samples // LANES
    return pl.pallas_call(
        functools.partial(own_kernel, len(pieces), len(received)),
        grid=(chans,),
        in_specs=[pl.BlockSpec((sources, rows, cols), lambda c: (0, 0, 0))]
        + [pl.BlockSpec((None, cols, samples), lambda c: (c, 0, 0)) for _ in pieces]
        + [pl.BlockSpec((None, rows, samples), lambda c: (c, 0, 0)) for _ in received],
        out_specs=[
            pl.BlockSpec((None, tiles, each, 2 * LANES), lambda c: (c, 0, 0, 0))
            for _ in range(blocks)
        ],
        out_shape=[
            jax.ShapeDtypeStruct((chans, tiles, each, 2 * LANES), jnp.bfloat16)
            for _ in range(blocks)
        ],
        name="own_beams",
        cost_estimate=pl.CostEstimate(
            flops=2 * chans * rows * sources * cols * samples,
            bytes_accessed=2 * (sources * rows * cols + chans * samples * (sources * cols + 3 * rows)),
            transcendentals=0,
        ),
    )(weights, *pieces, *received)


def spectrum_kernel(n_blocks, trial_block, last, *refs):
    me_ref = refs[0]
    in_refs = refs[1 : 1 + n_blocks]
    h_ref, dist_ref, delay_ref, acc_in = refs[1 + n_blocks : 5 + n_blocks]
    n_out = 1 + n_out_of(last)
    power_ref, *sum_refs = refs[5 + n_blocks : 5 + n_blocks + n_out]
    x_ref, c_ref, hot_ref, acc_ref = refs[5 + n_blocks + n_out :]
    step = pl.program_id(0)
    tiles, each, width = in_refs[0].shape
    all_tiles = n_blocks * tiles
    frames = all_tiles * (LANES // UPCH)
    trials = delay_ref.shape[0]

    x_ref[:each, :] = jnp.zeros((each, width), x_ref.dtype)
    for j, in_ref in enumerate(in_refs):
        block = lax.rem(me_ref[0] + (n_blocks - j), n_blocks)
        start = pl.multiple_of((1 + block * tiles) * each, each)
        x_ref[pl.ds(start, tiles * each), :] = in_ref[...].reshape(tiles * each, width)
    spectra = jnp.dot(x_ref[each:, :], h_ref[1], preferred_element_type=jnp.float32) + jnp.dot(
        x_ref[: all_tiles * each, :], h_ref[0], preferred_element_type=jnp.float32
    )
    real = spectra[:, :LANES] + spectra[:, 2 * LANES : 3 * LANES]
    imag = spectra[:, LANES : 2 * LANES] + spectra[:, 3 * LANES :]
    power = real * real + imag * imag
    mean = power[:each]
    for i in range(1, all_tiles):
        mean = mean + power[i * each : (i + 1) * each]
    shift = LANES // 2
    while shift >= UPCH:
        mean = mean + pltpu.roll(mean, shift, 1)
        shift //= 2
    mean = mean * (1.0 / frames)
    for i in range(all_tiles):
        lanes = slice(i * LANES, (i + 1) * LANES)
        tile = power[i * each : (i + 1) * each]
        power_ref[:, lanes] = tile
        centred = tile - mean
        high = centred.astype(jnp.bfloat16)
        c_ref[:each, lanes] = high
        c_ref[each:, lanes] = (centred - high.astype(jnp.float32)).astype(jnp.bfloat16)

    @pl.when(step == 0)
    def _():
        acc_ref[...] = jnp.zeros(acc_ref.shape, jnp.float32)

    def trial_group(g, carry):
        for i in range(all_tiles):
            lanes = slice(i * LANES, (i + 1) * LANES)
            dist = dist_ref[:, lanes]
            for d in range(trial_block):
                wanted = delay_ref[pl.ds(g * trial_block + d, 1), :]
                hot_ref[d * frames : (d + 1) * frames, lanes] = jnp.where(
                    dist == wanted, 1.0, 0.0
                ).astype(jnp.bfloat16)
        rows = pl.ds(pl.multiple_of(g * (trial_block * frames), trial_block * frames), trial_block * frames)
        acc_ref[rows, :] += lax.dot_general(
            hot_ref[...], c_ref[...], (((1,), (1,)), ((), ())), preferred_element_type=jnp.float32
        )
        return carry

    lax.fori_loop(0, trials // trial_block, trial_group, 0)

    @pl.when(step == pl.num_programs(0) - 1)
    def _():
        rows = acc_ref.shape[0] // len(sum_refs)
        for s, sum_ref in enumerate(sum_refs):
            part = slice(s * rows, (s + 1) * rows)
            total = acc_ref[part, :each] + acc_ref[part, each:] + acc_in[part, :]
            sum_ref[...] = total.astype(sum_ref.dtype)


def n_out_of(last):
    return last if last else 1


def spectrum(me, blocks, matrices, distance, delay_rows, start, sums, last):
    chans, tiles, each, width = blocks[0].shape
    samples = len(blocks) * tiles * LANES
    frames = samples // UPCH
    trials = delay_rows.shape[1]
    trial_block = math.gcd(trials, 8)
    n_sums = n_out_of(last)
    rows = trials * frames // n_sums
    whole = lambda shape: pl.BlockSpec(shape, lambda c, me: (0,) * len(shape))
    out = pl.pallas_call(
        functools.partial(spectrum_kernel, len(blocks), trial_block, last),
        grid_spec=pltpu.PrefetchScalarGridSpec(
            num_scalar_prefetch=1,
            grid=(chans,),
            in_specs=[
                pl.BlockSpec((None, tiles, each, width), lambda c, me: (c, 0, 0, 0)) for _ in blocks
            ]
            + [
                whole(matrices.shape),
                whole(distance.shape),
                pl.BlockSpec((None, trials, LANES), lambda c, me: (start + c, 0, 0)),
                whole(sums.shape),
            ],
            out_specs=[pl.BlockSpec((None, each, samples), lambda c, me: (c, 0, 0))]
            + [whole((rows, each)) for _ in range(n_sums)],
            scratch_shapes=[
                pltpu.VMEM(((1 + len(blocks) * tiles) * each, width), jnp.bfloat16),
                pltpu.VMEM((2 * each, samples), jnp.bfloat16),
                pltpu.VMEM((trial_block * frames, samples), jnp.bfloat16),
                pltpu.VMEM((trials * frames, 2 * each), jnp.float32),
            ],
        ),
        out_shape=[jax.ShapeDtypeStruct((chans, each, samples), jnp.float32)]
        + [
            jax.ShapeDtypeStruct((rows, each), jnp.bfloat16 if s else jnp.float32)
            for s in range(n_sums)
        ],
        name="spectrum",
        cost_estimate=pl.CostEstimate(
            flops=4 * chans * each * samples * (trials * frames + 8 * LANES),
            bytes_accessed=8 * chans * each * samples,
            transcendentals=0,
        ),
    )(me, *blocks, matrices, distance, delay_rows, sums)
    return out[0], out[1:]


def chunk_sizes(count):
    quarter = max(1, count // 4)
    sizes = []
    while sum(sizes) < count:
        sizes.append(min(quarter, count - sum(sizes)))
    return sizes


def per_device(voltages, positions, delays):
    places = BEAMS // 4
    n_chan = lax.axis_size("channel")
    n_time = lax.axis_size("tm")
    n_beam = lax.axis_size("beam")
    my_chan = lax.axis_index("channel")
    my_time = lax.axis_index("tm")
    my_beam = lax.axis_index("beam")
    _, feeds, channels, samples = voltages.shape
    own_channels = channels // n_chan
    half_beams = BEAMS // n_beam
    own_count = half_beams // n_time
    frames = n_time * samples // UPCH
    trials = delays.shape[0]
    sizes = chunk_sizes(own_channels)
    starts = [sum(sizes[:i]) for i in range(len(sizes))]

    by_channel = jnp.transpose(voltages, (2, 0, 1, 3)).reshape(channels, 2 * feeds, samples)
    pieces = []
    for start, size in zip(starts, sizes):
        chunk = []
        for s in range(n_chan):
            base = (my_chan + s) % n_chan * own_channels + start
            piece = lax.dynamic_slice_in_dim(by_channel, base, size, 0)
            chunk.append(ring(piece, "channel", s) if s else piece)
        pieces.append(chunk)

    grouped = positions.reshape(n_beam, n_chan, feeds)[my_beam]
    order = (my_chan - jnp.arange(n_chan)) % n_chan
    near = grouped[order].reshape(-1)
    block_ids = (my_time + jnp.arange(n_time)) % n_time
    local_ids = (block_ids[:, None] * own_count + jnp.arange(own_count)[None, :]).reshape(-1)
    weights = []
    for s in range(n_beam):
        beam_ids = (my_beam + s) % n_beam * half_beams + local_ids
        w_real, w_imag = steering(near, beam_ids, places, positions.shape[0])
        shape = (half_beams, n_chan, feeds)
        w_real = jnp.transpose(w_real.reshape(shape), (1, 0, 2))
        w_imag = jnp.transpose(w_imag.reshape(shape), (1, 0, 2))
        weights.append(
            jnp.concatenate(
                [
                    jnp.concatenate([w_real, -w_imag], axis=2),
                    jnp.concatenate([w_imag, w_real], axis=2),
                ],
                axis=1,
            )
        )

    matrices = jnp.asarray(filter_matrices())
    distance = jnp.asarray(frame_distance(frames))
    trial_order = (my_chan + jnp.arange(n_chan)) % n_chan
    delay_rows = delays.reshape(n_chan, trials // n_chan, own_channels, UPCH)[trial_order]
    delay_rows = jnp.transpose(delay_rows, (2, 0, 1, 3)).reshape(own_channels, trials, UPCH)
    delay_rows = jnp.tile(delay_rows, (1, 1, LANES // UPCH))
    me = my_time.astype(jnp.int32).reshape(1)

    powers = []
    sums = jnp.zeros((trials * frames, own_count), jnp.float32)
    for index, chunk in enumerate(pieces):
        received = [
            ring(beam_partial(weights[s], chunk), "beam", s) for s in range(1, n_beam)
        ]
        blocks = own_beams(weights[0], chunk, received, n_time)
        blocks = [ring(block, "tm", j) if j else block for j, block in enumerate(blocks)]
        last = n_chan if index == len(pieces) - 1 else 0
        power, out_sums = spectrum(
            me, blocks, matrices, distance, delay_rows, starts[index], sums, last
        )
        powers.append(power)
        sums = out_sums[0]
    total = sums
    for s in range(1, n_chan):
        total = total + ring(out_sums[s], "channel", s).astype(jnp.float32)
    total = total * (1.0 / math.sqrt(FINE))
    dedispersed = jnp.transpose(
        total.reshape(trials // n_chan, frames, own_count), (2, 0, 1)
    )
    intensity = jnp.transpose(jnp.concatenate(powers, axis=0), (1, 0, 2))
    return (intensity, dedispersed)


def solution(mesh):
    return jax.shard_map(
        per_device,
        mesh=mesh,
        in_specs=(P(None, ("beam", "channel"), None, "tm"), P(), P(None, "channel")),
        out_specs=(P(("beam", "tm"), "channel", None), P(("beam", "tm"), "channel", None)),
        check_vma=False,
    )
```

```python
import functools
import math

import jax
import jax.numpy as jnp
import numpy as np
from jax import lax
from jax.experimental import pallas as pl
from jax.experimental.pallas import tpu as pltpu
from jax.sharding import PartitionSpec as P


BEAMS = 1024
UPCH = 16
TAPS = 8
FINE = 1024
LANES = 128

TWO_PI = 2.0 * math.pi


def ring(value, axis, shift):
    count = lax.axis_size(axis)
    return lax.ppermute(value, axis, [(i, (i + shift) % count) for i in range(count)])


def stride(turn, parity, count):
    return 1 + (turn + 1 + 2 * parity) % (count - 1)


def partner(place, step, count):
    return place ^ step if count & (count - 1) == 0 else (step - place) % count


def exchange(value, turn):
    count, times = lax.axis_size("channel"), lax.axis_size("tm")
    pairs = [
        (i * times + t, partner(i, stride(turn, t % 2, count), count) * times + t)
        for i in range(count)
        for t in range(times)
    ]
    return lax.ppermute(value, ("channel", "tm"), pairs)


def steering(positions, beam_ids, places, feed_count):
    beam_east = beam_ids // places
    beam_north = beam_ids % places
    cylinder = positions // places
    along_row = positions % places
    coarse = (beam_east[:, None] * cylinder[None, :]) * (places // 4)
    steps = (coarse + beam_north[:, None] * along_row[None, :]) & (places - 1)
    quarter = places // 4
    side = (steps + quarter // 2) // quarter
    angle = (steps - side * quarter).astype(jnp.float32) * (TWO_PI / places)
    square = angle * angle
    sine = angle * (
        1.0 + square * (-1.0 / 6 + square * (1.0 / 120 + square * (-1.0 / 5040 + square / 362880)))
    )
    cosine = 1.0 + square * (
        -0.5 + square * (1.0 / 24 + square * (-1.0 / 720 + square * (1.0 / 40320 - square / 3628800)))
    )
    odd = (side & 1) == 1
    cos_part = jnp.where(odd, sine, cosine)
    sin_part = jnp.where(odd, cosine, sine)
    norm_scale = 1.0 / math.sqrt(feed_count)
    cos_sign = jnp.where(((side + 1) & 2) == 0, norm_scale, -norm_scale)
    sin_sign = jnp.where((side & 2) == 0, norm_scale, -norm_scale)
    w_real = (cos_part * cos_sign).astype(jnp.bfloat16)
    w_imag = (-sin_part * sin_sign).astype(jnp.bfloat16)
    return w_real, w_imag


def filter_matrices():
    length = TAPS * UPCH
    index = np.arange(length, dtype=np.float64)
    taper = np.sinc((index - (length - 1) / 2.0) / UPCH) * (
        0.5 - 0.5 * np.cos(TWO_PI * (index + 0.5) / length)
    )
    taper = taper / np.sqrt(np.sum(taper * taper))
    frames = LANES // UPCH
    mats = []
    for first in (-LANES, 0):
        sample = np.arange(first, first + LANES)
        inner = sample % UPCH
        tap = (sample - inner)[:, None] // UPCH - np.arange(frames)[None, :] + TAPS - 1
        inside = (tap >= 0) & (tap < TAPS)
        gain = np.where(inside, taper[np.clip(tap, 0, TAPS - 1) * UPCH + inner[:, None]], 0.0)
        phase = TWO_PI * (inner[:, None] * np.arange(UPCH)[None, :] % UPCH) / UPCH
        real = (gain[:, :, None] * np.cos(phase)[:, None, :]).reshape(LANES, LANES)
        imag = (gain[:, :, None] * -np.sin(phase)[:, None, :]).reshape(LANES, LANES)
        full = np.concatenate(
            [np.concatenate([real, imag], axis=1), np.concatenate([-imag, real], axis=1)], axis=0
        )
        high = full.astype(jnp.bfloat16)
        low = (full - high.astype(np.float64)).astype(jnp.bfloat16)
        mats.append(np.concatenate([high, low], axis=1))
    return np.stack(mats)


def frame_distance(frames):
    row = np.arange(frames)[:, None]
    col = np.arange(frames * UPCH)[None, :] // UPCH
    return ((row - col) % frames).astype(np.int32)


def spread_kernel(index_ref, v_ref, order_ref, *out_refs):
    step, width, samples = v_ref.shape
    rows = order_ref.shape[0]
    take = rows // width
    for f in range(step // take):
        part = v_ref[f * take : (f + 1) * take].reshape(rows, samples)
        moved = jnp.dot(order_ref[...], part, preferred_element_type=jnp.float32).astype(v_ref.dtype)
        c = 0
        for out_ref in out_refs:
            for i in range(out_ref.shape[0]):
                out_ref[i, f * take : (f + 1) * take, :] = moved[c * take : (c + 1) * take]
                c += 1


def spread(voltages, index, sizes):
    parts, feeds, _, samples = voltages.shape
    width = sum(sizes)
    take = math.gcd(feeds, 256 // width)
    step = math.gcd(feeds, 8 * take)
    cuts = feeds // step
    rows = take * width
    order = np.zeros((rows, rows), np.float32)
    for c in range(width):
        for f in range(take):
            order[c * take + f, f * width + c] = 1.0
    return pl.pallas_call(
        spread_kernel,
        grid_spec=pltpu.PrefetchScalarGridSpec(
            num_scalar_prefetch=1,
            grid=(parts, cuts),
            in_specs=[
                pl.BlockSpec((None, step, width, samples), lambda r, f, index: (r, f, index[0], 0)),
                pl.BlockSpec((rows, rows), lambda r, f, index: (0, 0)),
            ],
            out_specs=[
                pl.BlockSpec((size, step, samples), lambda r, f, index: (0, r * cuts + f, 0))
                for size in sizes
            ],
        ),
        out_shape=[
            jax.ShapeDtypeStruct((size, parts * feeds, samples), voltages.dtype) for size in sizes
        ],
        name="spread",
    )(index, voltages, jnp.asarray(order, voltages.dtype))


def partial_kernel(*refs):
    w_ref, *v_refs, _, out_ref = refs
    total = None
    for s, v_ref in enumerate(v_refs):
        part = jnp.dot(w_ref[s], v_ref[...], preferred_element_type=jnp.float32)
        total = part if total is None else total + part
    out_ref[...] = total.astype(out_ref.dtype)


def after():
    return pl.BlockSpec(memory_space=pl.ANY)


def beam_partial(weights, pieces, token):
    sources, rows, cols = weights.shape
    chans, _, samples = pieces[0].shape
    return pl.pallas_call(
        partial_kernel,
        grid=(chans,),
        in_specs=[pl.BlockSpec((sources, rows, cols), lambda c: (0, 0, 0))]
        + [pl.BlockSpec((None, cols, samples), lambda c: (c, 0, 0)) for _ in pieces]
        + [after()],
        out_specs=pl.BlockSpec((None, rows, samples), lambda c: (c, 0, 0)),
        out_shape=jax.ShapeDtypeStruct((chans, rows, samples), jnp.bfloat16),
        name="beam_partial",
        cost_estimate=pl.CostEstimate(
            flops=2 * chans * rows * sources * cols * samples,
            bytes_accessed=2 * (sources * rows * cols + chans * samples * (sources * cols + rows)),
            transcendentals=0,
        ),
    )(weights, *pieces, token)


def own_kernel(n_pieces, n_received, *refs):
    w_ref = refs[0]
    v_refs = refs[1 : 1 + n_pieces]
    r_refs = refs[1 + n_pieces : 1 + n_pieces + n_received]
    out_refs = refs[2 + n_pieces + n_received :]
    total = None
    for s, v_ref in enumerate(v_refs):
        part = jnp.dot(w_ref[s], v_ref[...], preferred_element_type=jnp.float32)
        total = part if total is None else total + part
    for r_ref in r_refs:
        total = total + r_ref[...].astype(jnp.float32)
    beams = total.astype(jnp.bfloat16)
    held = beams.shape[0] // 2
    each = held // len(out_refs)
    for j, out_ref in enumerate(out_refs):
        for a in range(out_ref.shape[0]):
            lanes = slice(a * LANES, (a + 1) * LANES)
            out_ref[a, :, :LANES] = beams[j * each : (j + 1) * each, lanes]
            out_ref[a, :, LANES:] = beams[held + j * each : held + (j + 1) * each, lanes]


def own_beams(weights, pieces, received, blocks, token):
    sources, rows, cols = weights.shape
    chans, _, samples = pieces[0].shape
    each = rows // 2 // blocks
    tiles = samples // LANES
    return pl.pallas_call(
        functools.partial(own_kernel, len(pieces), len(received)),
        grid=(chans,),
        in_specs=[pl.BlockSpec((sources, rows, cols), lambda c: (0, 0, 0))]
        + [pl.BlockSpec((None, cols, samples), lambda c: (c, 0, 0)) for _ in pieces]
        + [pl.BlockSpec((None, rows, samples), lambda c: (c, 0, 0)) for _ in received]
        + [after()],
        out_specs=[
            pl.BlockSpec((None, tiles, each, 2 * LANES), lambda c: (c, 0, 0, 0))
            for _ in range(blocks)
        ],
        out_shape=[
            jax.ShapeDtypeStruct((chans, tiles, each, 2 * LANES), jnp.bfloat16)
            for _ in range(blocks)
        ],
        name="own_beams",
        cost_estimate=pl.CostEstimate(
            flops=2 * chans * rows * sources * cols * samples,
            bytes_accessed=2 * (sources * rows * cols + chans * samples * (sources * cols + 3 * rows)),
            transcendentals=0,
        ),
    )(weights, *pieces, *received, token)


def spectrum_kernel(n_blocks, trial_block, last, *refs):
    me_ref = refs[0]
    in_refs = refs[1 : 1 + n_blocks]
    h_ref, dist_ref, delay_ref, acc_in = refs[1 + n_blocks : 5 + n_blocks]
    n_out = 1 + n_out_of(last)
    power_ref, *sum_refs = refs[6 + n_blocks : 6 + n_blocks + n_out]
    x_ref, c_ref, hot_ref, acc_ref = refs[6 + n_blocks + n_out :]
    step = pl.program_id(0)
    tiles, each, width = in_refs[0].shape
    all_tiles = n_blocks * tiles
    frames = all_tiles * (LANES // UPCH)
    trials = delay_ref.shape[0]

    x_ref[:each, :] = jnp.zeros((each, width), x_ref.dtype)
    for j, in_ref in enumerate(in_refs):
        block = lax.rem(me_ref[0] + (n_blocks - j), n_blocks)
        start = pl.multiple_of((1 + block * tiles) * each, each)
        x_ref[pl.ds(start, tiles * each), :] = in_ref[...].reshape(tiles * each, width)
    spectra = jnp.dot(x_ref[each:, :], h_ref[1], preferred_element_type=jnp.float32) + jnp.dot(
        x_ref[: all_tiles * each, :], h_ref[0], preferred_element_type=jnp.float32
    )
    real = spectra[:, :LANES] + spectra[:, 2 * LANES : 3 * LANES]
    imag = spectra[:, LANES : 2 * LANES] + spectra[:, 3 * LANES :]
    power = real * real + imag * imag
    mean = power[:each]
    for i in range(1, all_tiles):
        mean = mean + power[i * each : (i + 1) * each]
    shift = LANES // 2
    while shift >= UPCH:
        mean = mean + pltpu.roll(mean, shift, 1)
        shift //= 2
    mean = mean * (1.0 / frames)
    for i in range(all_tiles):
        lanes = slice(i * LANES, (i + 1) * LANES)
        tile = power[i * each : (i + 1) * each]
        power_ref[:, lanes] = tile
        centred = tile - mean
        high = centred.astype(jnp.bfloat16)
        c_ref[:each, lanes] = high
        c_ref[each:, lanes] = (centred - high.astype(jnp.float32)).astype(jnp.bfloat16)

    @pl.when(step == 0)
    def _():
        acc_ref[...] = jnp.zeros(acc_ref.shape, jnp.float32)

    def trial_group(g, carry):
        for i in range(all_tiles):
            lanes = slice(i * LANES, (i + 1) * LANES)
            dist = dist_ref[:, lanes]
            for d in range(trial_block):
                wanted = delay_ref[pl.ds(g * trial_block + d, 1), :]
                hot_ref[d * frames : (d + 1) * frames, lanes] = jnp.where(
                    dist == wanted, 1.0, 0.0
                ).astype(jnp.bfloat16)
        rows = pl.ds(pl.multiple_of(g * (trial_block * frames), trial_block * frames), trial_block * frames)
        acc_ref[rows, :] += lax.dot_general(
            hot_ref[...], c_ref[...], (((1,), (1,)), ((), ())), preferred_element_type=jnp.float32
        )
        return carry

    lax.fori_loop(0, trials // trial_block, trial_group, 0)

    @pl.when(step == pl.num_programs(0) - 1)
    def _():
        rows = acc_ref.shape[0] // len(sum_refs)
        for s, sum_ref in enumerate(sum_refs):
            part = slice(s * rows, (s + 1) * rows)
            total = acc_ref[part, :each] + acc_ref[part, each:] + acc_in[part, :]
            sum_ref[...] = total.astype(sum_ref.dtype)


def n_out_of(last):
    return last if last else 1


def spectrum(me, blocks, matrices, distance, delay_rows, start, sums, last, token):
    chans, tiles, each, width = blocks[0].shape
    samples = len(blocks) * tiles * LANES
    frames = samples // UPCH
    trials = delay_rows.shape[1]
    trial_block = math.gcd(trials, 8)
    n_sums = n_out_of(last)
    rows = trials * frames // n_sums
    whole = lambda shape: pl.BlockSpec(shape, lambda c, me: (0,) * len(shape))
    out = pl.pallas_call(
        functools.partial(spectrum_kernel, len(blocks), trial_block, last),
        grid_spec=pltpu.PrefetchScalarGridSpec(
            num_scalar_prefetch=1,
            grid=(chans,),
            in_specs=[
                pl.BlockSpec((None, tiles, each, width), lambda c, me: (c, 0, 0, 0)) for _ in blocks
            ]
            + [
                whole(matrices.shape),
                whole(distance.shape),
                pl.BlockSpec((None, trials, LANES), lambda c, me: (start + c, 0, 0)),
                whole(sums.shape),
                after(),
            ],
            out_specs=[pl.BlockSpec((None, each, samples), lambda c, me: (c, 0, 0))]
            + [whole((rows, each)) for _ in range(n_sums)],
            scratch_shapes=[
                pltpu.VMEM(((1 + len(blocks) * tiles) * each, width), jnp.bfloat16),
                pltpu.VMEM((2 * each, samples), jnp.bfloat16),
                pltpu.VMEM((trial_block * frames, samples), jnp.bfloat16),
                pltpu.VMEM((trials * frames, 2 * each), jnp.float32),
            ],
        ),
        out_shape=[jax.ShapeDtypeStruct((chans, each, samples), jnp.float32)]
        + [
            jax.ShapeDtypeStruct((rows, each), jnp.bfloat16 if s else jnp.float32)
            for s in range(n_sums)
        ],
        name="spectrum",
        cost_estimate=pl.CostEstimate(
            flops=4 * chans * each * samples * (trials * frames + 8 * LANES),
            bytes_accessed=8 * chans * each * samples,
            transcendentals=0,
        ),
    )(me, *blocks, matrices, distance, delay_rows, sums, token)
    return out[0], out[1:]


def place_kernel(n_chunks, *refs):
    out_ref = refs[-1]
    c = 0
    for in_ref in refs[:n_chunks]:
        for i in range(in_ref.shape[0]):
            out_ref[:, c, :] = in_ref[i]
            c += 1


def place(chunks, group, channels, held):
    _, beams, samples = chunks[0].shape
    width = sum(chunk.shape[0] for chunk in chunks)
    step = math.gcd(beams, 16)
    shape = (beams, channels, samples)
    return pl.pallas_call(
        functools.partial(place_kernel, len(chunks)),
        grid=(beams // step,),
        in_specs=[pl.BlockSpec((chunk.shape[0], step, samples), lambda b: (0, b, 0)) for chunk in chunks]
        + [pl.BlockSpec(memory_space=pl.ANY) for _ in held],
        out_specs=pl.BlockSpec((step, width, samples), lambda b: (b, group, 0)),
        out_shape=jax.ShapeDtypeStruct(shape, jnp.float32),
        input_output_aliases={len(chunks): 0} if held else {},
        name="place",
    )(*chunks, *held)


def chunk_sizes(count):
    eighth = count // 8
    if not eighth:
        return [1] * count
    rest = count - 7 * eighth
    small = max(1, rest // 2)
    return [eighth] * 7 + [rest - small, small]


def grouped_sizes(sizes, block):
    groups, filled = [[]], 0
    for size in sizes:
        groups[-1].append(size)
        filled += size
        if filled > block:
            return None
        if filled == block:
            groups.append([])
            filled = 0
    return groups[:-1] if filled == 0 else None


def per_device(voltages, positions, delays):
    places = BEAMS // 4
    n_chan = lax.axis_size("channel")
    n_time = lax.axis_size("tm")
    n_beam = lax.axis_size("beam")
    my_chan = lax.axis_index("channel")
    my_time = lax.axis_index("tm")
    my_beam = lax.axis_index("beam")
    _, feeds, channels, samples = voltages.shape
    own_channels = channels // n_chan
    half_beams = BEAMS // n_beam
    own_count = half_beams // n_time
    frames = n_time * samples // UPCH
    trials = delays.shape[0]
    sizes = chunk_sizes(own_channels)
    starts = [sum(sizes[:i]) for i in range(len(sizes))]

    groups = grouped_sizes(sizes, 8)
    targets = [my_chan] + [
        partner(my_chan, stride(turn, my_time % 2, n_chan), n_chan) for turn in range(n_chan - 1)
    ]
    by_target = [[] for _ in targets]
    if groups is None:
        by_channel = jnp.transpose(voltages, (2, 0, 1, 3)).reshape(channels, 2 * feeds, samples)
        for start, size in zip(starts, sizes):
            for s, target in enumerate(targets):
                piece = lax.dynamic_slice_in_dim(by_channel, target * own_channels + start, size, 0)
                by_target[s].append(piece)
    else:
        for g, group in enumerate(groups):
            for s in [*range(1, n_chan), 0]:
                index = targets[s] * (own_channels // 8) + g
                by_target[s] += spread(voltages, index.astype(jnp.int32).reshape(1), group)
    pieces = []
    for i in range(len(sizes)):
        chunk = [by_target[0][i]]
        for s in range(1, n_chan):
            chunk.append(exchange(by_target[s][i], s - 1))
        pieces.append(chunk)
    leaving = [by_target[s][0] for s in range(1, n_chan)]
    positions, _ = lax.optimization_barrier((positions, leaving))

    grouped = positions.reshape(n_beam, n_chan, feeds)[my_beam]
    near = grouped[jnp.stack(targets)].reshape(-1)
    block_ids = (my_time + jnp.arange(n_time)) % n_time
    local_ids = (block_ids[:, None] * own_count + jnp.arange(own_count)[None, :]).reshape(-1)
    weights = []
    for s in range(n_beam):
        beam_ids = (my_beam + s) % n_beam * half_beams + local_ids
        w_real, w_imag = steering(near, beam_ids, places, positions.shape[0])
        shape = (half_beams, n_chan, feeds)
        w_real = jnp.transpose(w_real.reshape(shape), (1, 0, 2))
        w_imag = jnp.transpose(w_imag.reshape(shape), (1, 0, 2))
        weights.append(
            jnp.concatenate(
                [
                    jnp.concatenate([w_real, -w_imag], axis=2),
                    jnp.concatenate([w_imag, w_real], axis=2),
                ],
                axis=1,
            )
        )

    matrices = jnp.asarray(filter_matrices())
    distance = jnp.asarray(frame_distance(frames))
    trial_order = (my_chan + jnp.arange(n_chan)) % n_chan
    delay_rows = delays.reshape(n_chan, trials // n_chan, own_channels, UPCH)[trial_order]
    delay_rows = jnp.transpose(delay_rows, (2, 0, 1, 3)).reshape(own_channels, trials, UPCH)
    delay_rows = jnp.tile(delay_rows, (1, 1, LANES // UPCH))
    me = my_time.astype(jnp.int32).reshape(1)

    powers = []
    sums = jnp.zeros((trials * frames, own_count), jnp.float32)
    received, blocks = {}, {}
    last = len(pieces) - 1
    token = by_target[-1][-1]
    for step in range(len(pieces) + 2):
        index = step
        if index <= last:
            received[index] = []
            for s in range(1, n_beam):
                token = beam_partial(weights[s], pieces[index], token)
                received[index].append(ring(token, "beam", s))
        index = step - 1
        if 0 <= index <= last:
            turned = own_beams(weights[0], pieces[index], received[index], n_time, token)
            token = turned[0]
            blocks[index] = [turned[0]]
            for j in range(1, n_time):
                blocks[index].append(ring(turned[j], "tm", j))
        index = step - 2
        if 0 <= index:
            power, out_sums = spectrum(
                me,
                blocks[index],
                matrices,
                distance,
                delay_rows,
                starts[index],
                sums,
                n_chan if index == last else 0,
                token,
            )
            powers.append(power)
            sums = out_sums[0]
            token = power
    total = sums
    for s in range(1, n_chan):
        total = total + ring(out_sums[s], "channel", s).astype(jnp.float32)
    total = total * (1.0 / math.sqrt(FINE))
    dedispersed = jnp.transpose(
        total.reshape(trials // n_chan, frames, own_count), (2, 0, 1)
    )
    if groups is None:
        intensity = jnp.transpose(jnp.concatenate(powers, axis=0), (1, 0, 2))
    else:
        held = []
        for g, group in enumerate(groups):
            held = [place(powers[: len(group)], g, own_channels, held)]
            powers = powers[len(group) :]
        intensity = held[0]
    return (intensity, dedispersed)


def solution(mesh):
    return jax.shard_map(
        per_device,
        mesh=mesh,
        in_specs=(P(None, ("beam", "channel"), None, "tm"), P(), P(None, "channel")),
        out_specs=(P(("beam", "tm"), "channel", None), P(("beam", "tm"), "channel", None)),
        check_vma=False,
    )
```

```python
import functools
import math

import jax
import jax.numpy as jnp
import numpy as np
from jax import lax
from jax.experimental import pallas as pl
from jax.experimental.pallas import tpu as pltpu
from jax.sharding import PartitionSpec as P


BEAMS = 1024
UPCH = 16
TAPS = 8
FINE = 1024
LANES = 128

TWO_PI = 2.0 * math.pi


def ring(value, axis, shift):
    count = lax.axis_size(axis)
    return lax.ppermute(value, axis, [(i, (i + shift) % count) for i in range(count)])


def stride(turn, parity, count):
    return 1 + (turn + 1 + 2 * parity) % (count - 1)


def partner(place, step, count):
    return place ^ step if count & (count - 1) == 0 else (step - place) % count


def exchange(value, turn):
    count, times = lax.axis_size("channel"), lax.axis_size("tm")
    pairs = [
        (i * times + t, partner(i, stride(turn, t % 2, count), count) * times + t)
        for i in range(count)
        for t in range(times)
    ]
    return lax.ppermute(value, ("channel", "tm"), pairs)


def steering(positions, beam_ids, places, feed_count):
    beam_east = beam_ids // places
    beam_north = beam_ids % places
    cylinder = positions // places
    along_row = positions % places
    coarse = (beam_east[:, None] * cylinder[None, :]) * (places // 4)
    steps = (coarse + beam_north[:, None] * along_row[None, :]) & (places - 1)
    quarter = places // 4
    side = (steps + quarter // 2) // quarter
    angle = (steps - side * quarter).astype(jnp.float32) * (TWO_PI / places)
    square = angle * angle
    sine = angle * (
        1.0 + square * (-1.0 / 6 + square * (1.0 / 120 + square * (-1.0 / 5040 + square / 362880)))
    )
    cosine = 1.0 + square * (
        -0.5 + square * (1.0 / 24 + square * (-1.0 / 720 + square * (1.0 / 40320 - square / 3628800)))
    )
    odd = (side & 1) == 1
    cos_part = jnp.where(odd, sine, cosine)
    sin_part = jnp.where(odd, cosine, sine)
    norm_scale = 1.0 / math.sqrt(feed_count)
    cos_sign = jnp.where(((side + 1) & 2) == 0, norm_scale, -norm_scale)
    sin_sign = jnp.where((side & 2) == 0, norm_scale, -norm_scale)
    w_real = (cos_part * cos_sign).astype(jnp.bfloat16)
    w_imag = (-sin_part * sin_sign).astype(jnp.bfloat16)
    return w_real, w_imag


def filter_matrices():
    length = TAPS * UPCH
    index = np.arange(length, dtype=np.float64)
    taper = np.sinc((index - (length - 1) / 2.0) / UPCH) * (
        0.5 - 0.5 * np.cos(TWO_PI * (index + 0.5) / length)
    )
    taper = taper / np.sqrt(np.sum(taper * taper))
    frames = LANES // UPCH
    mats = []
    for first in (-LANES, 0):
        sample = np.arange(first, first + LANES)
        inner = sample % UPCH
        tap = (sample - inner)[:, None] // UPCH - np.arange(frames)[None, :] + TAPS - 1
        inside = (tap >= 0) & (tap < TAPS)
        gain = np.where(inside, taper[np.clip(tap, 0, TAPS - 1) * UPCH + inner[:, None]], 0.0)
        phase = TWO_PI * (inner[:, None] * np.arange(UPCH)[None, :] % UPCH) / UPCH
        real = (gain[:, :, None] * np.cos(phase)[:, None, :]).reshape(LANES, LANES)
        imag = (gain[:, :, None] * -np.sin(phase)[:, None, :]).reshape(LANES, LANES)
        full = np.concatenate(
            [np.concatenate([real, imag], axis=1), np.concatenate([-imag, real], axis=1)], axis=0
        )
        high = full.astype(jnp.bfloat16)
        low = (full - high.astype(np.float64)).astype(jnp.bfloat16)
        mats.append(np.concatenate([high, low], axis=1))
    return np.stack(mats)


def frame_distance(frames):
    row = np.arange(frames)[:, None]
    col = np.arange(frames * UPCH)[None, :] // UPCH
    return ((row - col) % frames).astype(jnp.bfloat16)


def spread_kernel(index_ref, v_ref, order_ref, *out_refs):
    step, width, samples = v_ref.shape
    rows = order_ref.shape[0]
    take = rows // width
    for f in range(step // take):
        part = v_ref[f * take : (f + 1) * take].reshape(rows, samples)
        moved = jnp.dot(order_ref[...], part, preferred_element_type=jnp.float32).astype(v_ref.dtype)
        c = 0
        for out_ref in out_refs:
            for i in range(out_ref.shape[0]):
                out_ref[i, f * take : (f + 1) * take, :] = moved[c * take : (c + 1) * take]
                c += 1


def spread(voltages, index, sizes):
    parts, feeds, _, samples = voltages.shape
    width = sum(sizes)
    take = math.gcd(feeds, 256 // width)
    step = math.gcd(feeds, 8 * take)
    cuts = feeds // step
    rows = take * width
    order = np.zeros((rows, rows), np.float32)
    for c in range(width):
        for f in range(take):
            order[c * take + f, f * width + c] = 1.0
    return pl.pallas_call(
        spread_kernel,
        grid_spec=pltpu.PrefetchScalarGridSpec(
            num_scalar_prefetch=1,
            grid=(parts, cuts),
            in_specs=[
                pl.BlockSpec((None, step, width, samples), lambda r, f, index: (r, f, index[0], 0)),
                pl.BlockSpec((rows, rows), lambda r, f, index: (0, 0)),
            ],
            out_specs=[
                pl.BlockSpec((size, step, samples), lambda r, f, index: (0, r * cuts + f, 0))
                for size in sizes
            ],
        ),
        out_shape=[
            jax.ShapeDtypeStruct((size, parts * feeds, samples), voltages.dtype) for size in sizes
        ],
        name="spread",
    )(index, voltages, jnp.asarray(order, voltages.dtype))


def partial_kernel(*refs):
    w_ref, *v_refs, _, out_ref = refs
    total = None
    for s, v_ref in enumerate(v_refs):
        part = jnp.dot(w_ref[s], v_ref[...], preferred_element_type=jnp.float32)
        total = part if total is None else total + part
    out_ref[...] = total.astype(out_ref.dtype)


def after():
    return pl.BlockSpec(memory_space=pl.ANY)


def beam_partial(weights, pieces, token):
    sources, rows, cols = weights.shape
    chans, _, samples = pieces[0].shape
    return pl.pallas_call(
        partial_kernel,
        grid=(chans,),
        in_specs=[pl.BlockSpec((sources, rows, cols), lambda c: (0, 0, 0))]
        + [pl.BlockSpec((None, cols, samples), lambda c: (c, 0, 0)) for _ in pieces]
        + [after()],
        out_specs=pl.BlockSpec((None, rows, samples), lambda c: (c, 0, 0)),
        out_shape=jax.ShapeDtypeStruct((chans, rows, samples), jnp.bfloat16),
        name="beam_partial",
        cost_estimate=pl.CostEstimate(
            flops=2 * chans * rows * sources * cols * samples,
            bytes_accessed=2 * (sources * rows * cols + chans * samples * (sources * cols + rows)),
            transcendentals=0,
        ),
    )(weights, *pieces, token)


def own_kernel(n_pieces, n_received, *refs):
    w_ref = refs[0]
    v_refs = refs[1 : 1 + n_pieces]
    r_refs = refs[1 + n_pieces : 1 + n_pieces + n_received]
    out_refs = refs[2 + n_pieces + n_received :]
    total = None
    for s, v_ref in enumerate(v_refs):
        part = jnp.dot(w_ref[s], v_ref[...], preferred_element_type=jnp.float32)
        total = part if total is None else total + part
    for r_ref in r_refs:
        total = total + r_ref[...].astype(jnp.float32)
    beams = total.astype(jnp.bfloat16)
    held = beams.shape[0] // 2
    each = held // len(out_refs)
    for j, out_ref in enumerate(out_refs):
        for a in range(out_ref.shape[0]):
            lanes = slice(a * LANES, (a + 1) * LANES)
            out_ref[a, :, :LANES] = beams[j * each : (j + 1) * each, lanes]
            out_ref[a, :, LANES:] = beams[held + j * each : held + (j + 1) * each, lanes]


def own_beams(weights, pieces, received, blocks, token):
    sources, rows, cols = weights.shape
    chans, _, samples = pieces[0].shape
    each = rows // 2 // blocks
    tiles = samples // LANES
    return pl.pallas_call(
        functools.partial(own_kernel, len(pieces), len(received)),
        grid=(chans,),
        in_specs=[pl.BlockSpec((sources, rows, cols), lambda c: (0, 0, 0))]
        + [pl.BlockSpec((None, cols, samples), lambda c: (c, 0, 0)) for _ in pieces]
        + [pl.BlockSpec((None, rows, samples), lambda c: (c, 0, 0)) for _ in received]
        + [after()],
        out_specs=[
            pl.BlockSpec((None, tiles, each, 2 * LANES), lambda c: (c, 0, 0, 0))
            for _ in range(blocks)
        ],
        out_shape=[
            jax.ShapeDtypeStruct((chans, tiles, each, 2 * LANES), jnp.bfloat16)
            for _ in range(blocks)
        ],
        name="own_beams",
        cost_estimate=pl.CostEstimate(
            flops=2 * chans * rows * sources * cols * samples,
            bytes_accessed=2 * (sources * rows * cols + chans * samples * (sources * cols + 3 * rows)),
            transcendentals=0,
        ),
    )(weights, *pieces, *received, token)


def spectrum_kernel(n_blocks, trial_block, last, *refs):
    me_ref = refs[0]
    in_refs = refs[1 : 1 + n_blocks]
    h_ref, dist_ref, delay_ref, acc_in = refs[1 + n_blocks : 5 + n_blocks]
    n_out = 1 + n_out_of(last)
    power_ref, *sum_refs = refs[6 + n_blocks : 6 + n_blocks + n_out]
    x_ref, c_ref, hot_ref, acc_ref = refs[6 + n_blocks + n_out :]
    step = pl.program_id(0)
    tiles, each, width = in_refs[0].shape
    all_tiles = n_blocks * tiles
    frames = all_tiles * (LANES // UPCH)
    trials = delay_ref.shape[0]

    x_ref[:each, :] = jnp.zeros((each, width), x_ref.dtype)
    for j, in_ref in enumerate(in_refs):
        block = lax.rem(me_ref[0] + (n_blocks - j), n_blocks)
        start = pl.multiple_of((1 + block * tiles) * each, each)
        x_ref[pl.ds(start, tiles * each), :] = in_ref[...].reshape(tiles * each, width)
    spectra = jnp.dot(x_ref[each:, :], h_ref[1], preferred_element_type=jnp.float32) + jnp.dot(
        x_ref[: all_tiles * each, :], h_ref[0], preferred_element_type=jnp.float32
    )
    real = spectra[:, :LANES] + spectra[:, 2 * LANES : 3 * LANES]
    imag = spectra[:, LANES : 2 * LANES] + spectra[:, 3 * LANES :]
    power = real * real + imag * imag
    mean = power[:each]
    for i in range(1, all_tiles):
        mean = mean + power[i * each : (i + 1) * each]
    shift = LANES // 2
    while shift >= UPCH:
        mean = mean + pltpu.roll(mean, shift, 1)
        shift //= 2
    mean = mean * (1.0 / frames)
    for i in range(all_tiles):
        lanes = slice(i * LANES, (i + 1) * LANES)
        tile = power[i * each : (i + 1) * each]
        power_ref[:, lanes] = tile
        centred = tile - mean
        high = centred.astype(jnp.bfloat16)
        c_ref[:each, lanes] = high
        c_ref[each:, lanes] = (centred - high.astype(jnp.float32)).astype(jnp.bfloat16)

    @pl.when(step == 0)
    def _():
        acc_ref[...] = jnp.zeros(acc_ref.shape, jnp.float32)

    def trial_group(g, carry):
        for i in range(all_tiles):
            lanes = slice(i * LANES, (i + 1) * LANES)
            dist = dist_ref[:, lanes]
            for d in range(trial_block):
                wanted = delay_ref[pl.ds(g * trial_block + d, 1), :]
                wanted = jnp.broadcast_to(wanted, dist.shape).astype(jnp.bfloat16)
                hot_ref[d * frames : (d + 1) * frames, lanes] = jnp.where(
                    dist == wanted, jnp.bfloat16(1.0), jnp.bfloat16(0.0)
                )
        rows = pl.ds(pl.multiple_of(g * (trial_block * frames), trial_block * frames), trial_block * frames)
        acc_ref[rows, :] += lax.dot_general(
            hot_ref[...], c_ref[...], (((1,), (1,)), ((), ())), preferred_element_type=jnp.float32
        )
        return carry

    lax.fori_loop(0, trials // trial_block, trial_group, 0)

    @pl.when(step == pl.num_programs(0) - 1)
    def _():
        rows = acc_ref.shape[0] // len(sum_refs)
        for s, sum_ref in enumerate(sum_refs):
            part = slice(s * rows, (s + 1) * rows)
            total = acc_ref[part, :each] + acc_ref[part, each:] + acc_in[part, :]
            sum_ref[...] = total.astype(sum_ref.dtype)


def n_out_of(last):
    return last if last else 1


def spectrum(me, blocks, matrices, distance, delay_rows, start, sums, last, token):
    chans, tiles, each, width = blocks[0].shape
    samples = len(blocks) * tiles * LANES
    frames = samples // UPCH
    trials = delay_rows.shape[1]
    trial_block = math.gcd(trials, 8)
    n_sums = n_out_of(last)
    rows = trials * frames // n_sums
    whole = lambda shape: pl.BlockSpec(shape, lambda c, me: (0,) * len(shape))
    out = pl.pallas_call(
        functools.partial(spectrum_kernel, len(blocks), trial_block, last),
        grid_spec=pltpu.PrefetchScalarGridSpec(
            num_scalar_prefetch=1,
            grid=(chans,),
            in_specs=[
                pl.BlockSpec((None, tiles, each, width), lambda c, me: (c, 0, 0, 0)) for _ in blocks
            ]
            + [
                whole(matrices.shape),
                whole(distance.shape),
                pl.BlockSpec((None, trials, LANES), lambda c, me: (start + c, 0, 0)),
                whole(sums.shape),
                after(),
            ],
            out_specs=[pl.BlockSpec((None, each, samples), lambda c, me: (c, 0, 0))]
            + [whole((rows, each)) for _ in range(n_sums)],
            scratch_shapes=[
                pltpu.VMEM(((1 + len(blocks) * tiles) * each, width), jnp.bfloat16),
                pltpu.VMEM((2 * each, samples), jnp.bfloat16),
                pltpu.VMEM((trial_block * frames, samples), jnp.bfloat16),
                pltpu.VMEM((trials * frames, 2 * each), jnp.float32),
            ],
        ),
        out_shape=[jax.ShapeDtypeStruct((chans, each, samples), jnp.float32)]
        + [
            jax.ShapeDtypeStruct((rows, each), jnp.bfloat16 if s else jnp.float32)
            for s in range(n_sums)
        ],
        name="spectrum",
        cost_estimate=pl.CostEstimate(
            flops=4 * chans * each * samples * (trials * frames + 8 * LANES),
            bytes_accessed=8 * chans * each * samples,
            transcendentals=0,
        ),
    )(me, *blocks, matrices, distance, delay_rows, sums, token)
    return out[0], out[1:]


def place_kernel(n_chunks, *refs):
    out_ref = refs[-1]
    c = 0
    for in_ref in refs[:n_chunks]:
        for i in range(in_ref.shape[0]):
            out_ref[:, c, :] = in_ref[i]
            c += 1


def place(chunks, group, channels, held):
    _, beams, samples = chunks[0].shape
    width = sum(chunk.shape[0] for chunk in chunks)
    step = math.gcd(beams, 16)
    shape = (beams, channels, samples)
    return pl.pallas_call(
        functools.partial(place_kernel, len(chunks)),
        grid=(beams // step,),
        in_specs=[pl.BlockSpec((chunk.shape[0], step, samples), lambda b: (0, b, 0)) for chunk in chunks]
        + [pl.BlockSpec(memory_space=pl.ANY) for _ in held],
        out_specs=pl.BlockSpec((step, width, samples), lambda b: (b, group, 0)),
        out_shape=jax.ShapeDtypeStruct(shape, jnp.float32),
        input_output_aliases={len(chunks): 0} if held else {},
        name="place",
    )(*chunks, *held)


def chunk_sizes(count):
    eighth = max(1, count // 8)
    sizes = [eighth] * (count // eighth)
    return sizes + [count - sum(sizes)] if sum(sizes) < count else sizes


def grouped_sizes(sizes, block):
    groups, filled = [[]], 0
    for size in sizes:
        groups[-1].append(size)
        filled += size
        if filled > block:
            return None
        if filled == block:
            groups.append([])
            filled = 0
    return groups[:-1] if filled == 0 else None


def per_device(voltages, positions, delays):
    places = BEAMS // 4
    n_chan = lax.axis_size("channel")
    n_time = lax.axis_size("tm")
    n_beam = lax.axis_size("beam")
    my_chan = lax.axis_index("channel")
    my_time = lax.axis_index("tm")
    my_beam = lax.axis_index("beam")
    _, feeds, channels, samples = voltages.shape
    own_channels = channels // n_chan
    half_beams = BEAMS // n_beam
    own_count = half_beams // n_time
    frames = n_time * samples // UPCH
    trials = delays.shape[0]
    sizes = chunk_sizes(own_channels)
    starts = [sum(sizes[:i]) for i in range(len(sizes))]

    groups = grouped_sizes(sizes, 8)
    targets = [my_chan] + [
        partner(my_chan, stride(turn, my_time % 2, n_chan), n_chan) for turn in range(n_chan - 1)
    ]
    by_target = [[] for _ in targets]
    if groups is None:
        by_channel = jnp.transpose(voltages, (2, 0, 1, 3)).reshape(channels, 2 * feeds, samples)
        for start, size in zip(starts, sizes):
            for s, target in enumerate(targets):
                piece = lax.dynamic_slice_in_dim(by_channel, target * own_channels + start, size, 0)
                by_target[s].append(piece)
    else:
        for g, group in enumerate(groups):
            for s in [*range(1, n_chan), 0]:
                index = targets[s] * (own_channels // 8) + g
                by_target[s] += spread(voltages, index.astype(jnp.int32).reshape(1), group)
    pieces = []
    for i in range(len(sizes)):
        chunk = [by_target[0][i]]
        for s in range(1, n_chan):
            chunk.append(exchange(by_target[s][i], s - 1))
        pieces.append(chunk)
    leaving = [by_target[s][0] for s in range(1, n_chan)]
    positions, _ = lax.optimization_barrier((positions, leaving))

    grouped = positions.reshape(n_beam, n_chan, feeds)[my_beam]
    near = grouped[jnp.stack(targets)].reshape(-1)
    block_ids = (my_time + jnp.arange(n_time)) % n_time
    local_ids = (block_ids[:, None] * own_count + jnp.arange(own_count)[None, :]).reshape(-1)
    weights = []
    for s in range(n_beam):
        beam_ids = (my_beam + s) % n_beam * half_beams + local_ids
        w_real, w_imag = steering(near, beam_ids, places, positions.shape[0])
        shape = (half_beams, n_chan, feeds)
        w_real = jnp.transpose(w_real.reshape(shape), (1, 0, 2))
        w_imag = jnp.transpose(w_imag.reshape(shape), (1, 0, 2))
        weights.append(
            jnp.concatenate(
                [
                    jnp.concatenate([w_real, -w_imag], axis=2),
                    jnp.concatenate([w_imag, w_real], axis=2),
                ],
                axis=1,
            )
        )

    matrices = jnp.asarray(filter_matrices())
    distance = jnp.asarray(frame_distance(frames))
    trial_order = (my_chan + jnp.arange(n_chan)) % n_chan
    delay_rows = delays.reshape(n_chan, trials // n_chan, own_channels, UPCH)[trial_order]
    delay_rows = jnp.transpose(delay_rows, (2, 0, 1, 3)).reshape(own_channels, trials, UPCH)
    delay_rows = jnp.tile(delay_rows, (1, 1, LANES // UPCH)).astype(jnp.float32)
    me = my_time.astype(jnp.int32).reshape(1)

    powers, held, placed = [], [], 0
    sums = jnp.zeros((trials * frames, own_count), jnp.float32)
    received, blocks = {}, {}
    last = len(pieces) - 1
    token = by_target[-1][-1]
    for step in range(len(pieces) + 2):
        index = step
        if index <= last:
            received[index] = []
            for s in range(1, n_beam):
                token = beam_partial(weights[s], pieces[index], token)
                received[index].append(ring(token, "beam", s))
        index = step - 1
        if 0 <= index <= last:
            turned = own_beams(weights[0], pieces[index], received[index], n_time, token)
            token = turned[0]
            blocks[index] = [turned[0]]
            for j in range(1, n_time):
                blocks[index].append(ring(turned[j], "tm", j))
        index = step - 2
        if 0 <= index:
            power, out_sums = spectrum(
                me,
                blocks[index],
                matrices,
                distance,
                delay_rows,
                starts[index],
                sums,
                n_chan if index == last else 0,
                token,
            )
            powers.append(power)
            sums = out_sums[0]
            token = power
            if groups is not None and index < last and len(powers) == len(groups[placed]):
                held = [place(powers, placed, own_channels, held)]
                token = held[0]
                powers = []
                placed += 1
    total = sums
    for s in range(1, n_chan):
        total = total + ring(out_sums[s], "channel", s).astype(jnp.float32)
    total = total * (1.0 / math.sqrt(FINE))
    dedispersed = jnp.transpose(
        total.reshape(trials // n_chan, frames, own_count), (2, 0, 1)
    )
    if groups is None:
        intensity = jnp.transpose(jnp.concatenate(powers, axis=0), (1, 0, 2))
    else:
        intensity = place(powers, placed, own_channels, held)
    return (intensity, dedispersed)


def solution(mesh):
    return jax.shard_map(
        per_device,
        mesh=mesh,
        in_specs=(P(None, ("beam", "channel"), None, "tm"), P(), P(None, "channel")),
        out_specs=(P(("beam", "tm"), "channel", None), P(("beam", "tm"), "channel", None)),
        check_vma=False,
    )
```
